32 devices in a mesh: grp: 2 (over y), shard: 16 (over z, x, core).
Axes of the slice: x: 2, y: 2, z: 4, core: 2. Of those that a mesh axis runs over, the one named last changes fastest.
Arguments:
- points: bfloat16 [65536, 128], P(('grp', 'shard')), may hold values from -9 to 9
- sub_label: int32 [65536], P(('grp', 'shard')), may hold values from 0 to 511, as said below
- block_route: int32 [512, 1], P(('grp', 'shard')), may hold values from 0 to 1; in each aligned block of 16 rows (0 to 15, 16 to 31, ...) at most 8 rows name the same one
Outputs:
- centroids: float32 [2, 512, 128], P('grp')
- min_dist: float32 [65536], P(('grp', 'shard'))
- inertia: float32 [], replicated
The draws below stay inside these ranges and needn't reach their ends.
Inputs may be any that keep to these rules, and one draw needn't show every extreme that they name: `block_route`: of the 16 blocks of one device at most 8 name the same group. `sub_label`: A subcluster of a group may hold no points.
All inputs are finite; a program needn't handle non-finite values.
Results may differ from the reference program's by a relative error of at most 0.0003.
Values may be sent and summed in bfloat16 or wider, within the bound.
A program may use at most 64 MiB of HBM per device.

```python
import math
import jax
import jax.numpy as jnp
import numpy as np
from jax import lax

D = 128
K = 512
BLK_ROWS = 128
BLK_DEV = 16
MOST = 8
BLOCKS = 512
POINTS = 65536
N_GRP = 2


def draw_points(key, part):
    first = jax.random.fold_in(jax.random.fold_in(key, 11), 0)
    position = jnp.arange(POINTS, dtype=jnp.float32) / POINTS
    rising = 1.0 + (math.sqrt(3.0) - 1.0) * position
    base = jnp.clip(jax.random.normal(first, (POINTS, D), jnp.float32), -5.0, 5.0)
    return (base * rising[:, None]).astype(jnp.bfloat16)


def draw_sub_label(key, part):
    perm_key, first_key, second_key = jax.random.split(jax.random.fold_in(key, 23), 3)
    missing = max(K // 32, 1)
    live_count = K - missing
    inner_ids = (1 + jax.random.permutation(perm_key, K - 2)).astype(jnp.int32)
    live_ids = jnp.concatenate([jnp.array([0, K - 1], jnp.int32), inner_ids[:live_count - 2]])
    first_pick = jax.random.randint(first_key, (POINTS,), 0, live_count, jnp.int32)
    second_pick = jax.random.randint(second_key, (POINTS,), 0, live_count, jnp.int32)
    picked = jnp.minimum(first_pick, second_pick)
    return live_ids[picked].astype(jnp.int32)


def deal_out(own_key, own, number, rows, count, top, limit, slope):
    ranking = jax.random.permutation(own_key, count)
    crowded, ordinary = shares(count, rows * top, limit, slope, True), shares(count, rows * top, limit, slope, False)
    places = jnp.arange(count)

    def named(sizes, rotation):
        used = int((sizes > 0).sum())
        fixed = max(1, used // 4)
        passed = fixed + (places - fixed + rotation * (used - fixed)) % max(1, count - fixed)
        return jnp.zeros((count,), jnp.int32).at[ranking[jnp.where(places < fixed, places, passed)]].set(jnp.asarray(sizes, jnp.int32))

    sizes = jnp.where(number % 4 == 0, named(crowded, number // 4), named(ordinary, number - number // 4 - 1))
    mixed = jax.random.permutation(jax.random.fold_in(own, 3), count)
    donor, sink = mixed[0:count // 2 * 2:2], mixed[1:count // 2 * 2:2]
    slack = jnp.minimum(sizes[donor] - 1, limit - sizes[sink]) // 2
    slack = jnp.where((donor == ranking[0]) | (sink == ranking[0]) | (sizes[sink] == 0), 0, jnp.maximum(slack, 0))
    passed = jax.random.randint(jax.random.fold_in(own, 4), (count // 2,), 0, 1 << 20) % (slack + 1)
    sizes = sizes.at[donor].add(-passed).at[sink].add(passed)
    items = jnp.searchsorted(jnp.cumsum(sizes), jnp.arange(rows * top), side="right").astype(jnp.int32)
    table = items.reshape(top, rows).T
    table = table[jax.random.permutation(jax.random.fold_in(own, 1), rows)]
    rotation = jax.random.randint(jax.random.fold_in(own, 2), (rows, 1), 0, top)
    return jnp.take_along_axis(table, (jnp.arange(top)[None, :] + rotation) % top, axis=1)


def shares(amount, total, limit, slope, full):
    weights = [(1 << 20) // math.isqrt(rank ** slope) + 1 for rank in range(1, amount + 1)]
    largest = limit if full else min(limit, max(-(-total // amount), total * weights[0] // sum(weights)))
    least = 1 if total - largest >= amount - 1 else 0
    given, spare = [largest] + [least] * (amount - 1), total - largest - least * (amount - 1)
    while spare > 0:
        free = [i for i in range(1, amount) if given[i] < largest] or [i for i in range(1, amount) if given[i] < limit]
        pool, left = sum([weights[i] for i in free]), spare
        for i in free:
            addition = min(limit - given[i], max(1, left * weights[i] // pool), spare)
            given[i] = given[i] + addition
            spare = spare - addition
    return np.array(given)


def setup_inputs(seed: int = 0) -> dict:
    keys = jax.random.split(jax.random.key(seed), 4)
    points = draw_points(jax.random.fold_in(keys[3], 71), 0)
    sub_label = draw_sub_label(jax.random.fold_in(keys[3], 71), 0)
    block_route_keys = jax.random.split(jax.random.fold_in(keys[2], 1), BLOCKS // BLK_DEV)
    block_route_turns = jax.random.permutation(jax.random.fold_in(keys[2], 3), BLOCKS // BLK_DEV)
    block_route = jax.vmap(lambda own, number: deal_out(jax.random.fold_in(keys[2], 2), own, number, BLK_DEV, N_GRP, 1, MOST, 1))(block_route_keys, block_route_turns).reshape((BLOCKS, 1))
    return {"points": points, "sub_label": sub_label, "block_route": block_route}


def reference(points, sub_label, block_route):
    route = block_route[:, 0].astype(jnp.int32)
    row_group = jnp.repeat(route, BLK_ROWS)
    combined = (row_group * K + sub_label).astype(jnp.int32)
    sums = jax.ops.segment_sum(points.astype(jnp.float32), combined, num_segments=N_GRP * K)
    counts = jax.ops.segment_sum(jnp.ones(combined.shape, jnp.float32), combined, num_segments=N_GRP * K)
    centers = sums / jnp.maximum(counts, 1.0)[:, None]
    rounded = centers.astype(jnp.bfloat16)
    center_norm = (jnp.sum(rounded.astype(jnp.float32) ** 2, axis=1) / D).reshape(N_GRP, K)
    grouped = rounded.reshape(N_GRP, K, D)
    blocks = points.reshape(-1, BLK_ROWS, D)

    def nearest(item):
        sample_blk, which = item
        cross = lax.dot_general(sample_blk, grouped[which], (((1,), (1,)), ((), ())), preferred_element_type=jnp.float32)
        sample_f = sample_blk.astype(jnp.float32)
        self_norm = jnp.sum(sample_f * sample_f, axis=1) / D
        dist = self_norm[:, None] - (2.0 / D) * cross + center_norm[which][None, :]
        return jnp.min(dist, axis=1)

    min_dist = lax.map(nearest, (blocks, route)).reshape(-1)
    inertia = jnp.sum(min_dist) / POINTS
    return centers.reshape(N_GRP, K, D), min_dist, inertia
```

```python
import functools
import math

import jax
import jax.numpy as jnp
from jax import lax
from jax.experimental import pallas as pl
from jax.experimental.pallas import tpu as pltpu
from jax.sharding import PartitionSpec as P

K = 512
MESH = pl.DeviceIdType.MESH


def plan(shard):
    cores = 2 if shard % 2 == 0 else 1
    near = 2 if (shard // cores) % 2 == 0 else 1
    rest = shard // (cores * near)
    far = math.gcd(rest, K // (cores * near) // 8)
    return cores, near, far, rest // far


def kernel(dims, route_ref, pts_ref, lab_ref, cent_ref, dist_ref, inert_ref,
           aug, onehot, acc, recv_a, recv_b, recv_c, own_d, recv_d,
           f_own, f_oth, r_own, r_oth, cn_own, cn_oth, xn, ibuf,
           sa, ra, sb, rb, sc, rc, sd, rd, sgc, rgc, sgb, rgb, sga, rga, si, ri):
    G, S, C, X, Z, O, R = dims
    n = G * S
    total_points = pts_ref.shape[0] * n
    D = pts_ref.shape[1]
    nblk, width = lab_ref.shape
    half = X * Z * R
    g = lax.axis_index("grp")
    s = lax.axis_index("shard")
    c = lax.rem(s, C)
    x = lax.rem(s // C, X)
    z = lax.rem(s // (C * X), Z)
    o = s // (C * X * Z)

    def at(g_, c_, x_, z_, o_):
        return (g_, ((o_ * Z + z_) * X + x_) * C + c_)

    def up(v, d, m):
        return lax.rem(v + d, m)

    def down(v, d, m):
        return lax.rem(v + m - d, m)

    me = g * S + s
    barrier = pltpu.get_barrier_semaphore()

    def greet(i, _):
        t = lax.rem(me + i, n)
        pl.semaphore_signal(barrier, inc=1, device_id=(t // S, lax.rem(t, S)), device_id_type=MESH)
        return 0

    lax.fori_loop(1, n, greet, 0)

    aug[:, :D] = pts_ref[...]
    aug[:, D:] = jnp.ones((pts_ref.shape[0], D), jnp.bfloat16)
    rows = G * half
    row = lax.broadcasted_iota(jnp.int32, (rows, width), 0)
    base_ids = row // half * K + lax.rem(row, half)
    eye_r = (lax.broadcasted_iota(jnp.int32, (R, D), 0) == lax.broadcasted_iota(jnp.int32, (R, D), 1))

    def local_sums(core):
        for b in range(nblk):
            lab = lab_ref[b:b + 1, :] + (route_ref[b] * K - core * half)
            onehot[:, b * width:(b + 1) * width] = jnp.where(base_ids == lab, 1.0, 0.0).astype(jnp.bfloat16)
        res = jnp.dot(onehot[...], aug[...], preferred_element_type=jnp.float32)
        cnt = jnp.where(eye_r[None], res[:, D:].reshape(G * X * Z, R, D), 0.0)
        cnt = jnp.sum(cnt, axis=1, keepdims=True)
        acc[core, :, :, :, 0:R, :] = res[:, :D].reshape(G, X, Z, R, D)
        acc[core, :, :, :, R:R + 1, :] = cnt.reshape(G, X, Z, 1, D)

    def remote(src, dst, ssem, rsem, dev):
        return pltpu.make_async_remote_copy(
            src_ref=src, dst_ref=dst, send_sem=ssem, recv_sem=rsem, device_id=dev, device_id_type=MESH)

    live = pl.ds(0, R + 1)
    sent = []

    def go(cp):
        cp.start()
        sent.append(cp)
        return cp

    oc = C - 1 - c
    if C > 1:
        local_sums(oc)
    pl.semaphore_wait(barrier, n - 1)
    if C > 1:
        cp_a = go(remote(acc.at[oc, :, :, :, live], recv_a.at[:, :, :, live], sa, ra, at(g, oc, x, z, o)))
    local_sums(c)

    if C > 1:
        cp_a.wait_recv()
        acc[c, :, :, :, 0:R + 1, :] = acc[c, :, :, :, 0:R + 1, :] + recv_a[:, :, :, 0:R + 1, :]

    plane = [(dg, dx) for dg in range(G) for dx in range(X) if dg or dx]
    plane.sort(key=lambda t: -((t[0] > 0) + (t[1] > 0)))
    cps = []
    for i, (dg, dx) in enumerate(plane):
        tg, tx = up(g, dg, G), up(x, dx, X)
        cps.append(go(remote(acc.at[c, tg, tx, :, live], recv_b.at[i, :, live], sb.at[i], rb.at[i],
                             at(tg, c, tx, z, o))))

    eye = (lax.broadcasted_iota(jnp.int32, (width, width), 0) == lax.broadcasted_iota(jnp.int32, (width, width), 1))
    for b in range(nblk):
        p = pts_ref[b * width:(b + 1) * width, :].astype(jnp.float32)
        sq = jnp.sum(p * p, axis=1, keepdims=True)
        xn[b:b + 1, :] = jnp.sum(jnp.where(eye, sq, 0.0), axis=0, keepdims=True) / D

    for cp in cps:
        cp.wait_recv()
    tot = acc[c, g, x, :, 0:R + 1, :]
    for i in range(len(plane)):
        tot = tot + recv_b[i, :, 0:R + 1, :]
    acc[c, g, x, :, 0:R + 1, :] = tot

    cps = []
    for d in sorted(range(1, Z), key=lambda d: -min(d, Z - d)):
        tz = up(z, d, Z)
        cps.append(go(remote(acc.at[c, g, x, tz, live], recv_c.at[d - 1, live], sc.at[d - 1], rc.at[d - 1],
                             at(g, c, x, tz, o))))
    for cp in cps:
        cp.wait_recv()
    tot = acc[c, g, x, z, 0:R + 1, :]
    for d in range(1, Z):
        tot = tot + recv_c[d - 1, 0:R + 1, :]
    if O > 1:
        own_d[0:R + 1, :] = tot
        cps = []
        for d in range(1, O):
            cps.append(go(remote(own_d.at[live], recv_d.at[d - 1, live], sd.at[d - 1], rd.at[d - 1],
                                 at(g, c, x, z, up(o, d, O)))))
        for cp in cps:
            cp.wait_recv()
        for d in range(1, O):
            tot = tot + recv_d[d - 1, 0:R + 1, :]
    counts = jnp.sum(jnp.where(eye_r, tot[R:R + 1, :], 0.0), axis=1, keepdims=True)
    f_own[x, z] = tot[0:R] / jnp.maximum(counts, 1.0)

    def norm(r):
        r = r.astype(jnp.float32)
        return jnp.broadcast_to(jnp.sum(r * r, axis=1, keepdims=True) / D, r.shape)

    gather_c = [None]
    for d in range(1, Z):
        gather_c.append(go(remote(f_own.at[x, z], f_own.at[x, z], sgc.at[d - 1], rgc.at[d - 1],
                                  at(g, c, x, up(z, d, Z), o))))
    gather_b = []
    gather_a = []
    for d in range(Z):
        if d:
            gather_c[d].wait_recv()
        zz = down(z, d, Z)
        rounded = f_own[x, zz].astype(jnp.bfloat16)
        r_own[g, x, zz] = rounded
        for i, (dg, dx) in enumerate(plane):
            dev = at(up(g, dg, G), c, up(x, dx, X), z, o)
            if dg:
                src, dst = r_own.at[g, x, zz], r_own.at[g, x, zz]
            else:
                src, dst = f_own.at[x, zz], f_own.at[x, zz]
            gather_b.append((d, dg, dx, go(remote(src, dst, sgb.at[d, i], rgb.at[d, i], dev))))
        if C > 1:
            gather_a.append((d, 0, 0, go(remote(f_own.at[x, zz], f_oth.at[x, zz], sga.at[d, 0], rga.at[d, 0],
                                                at(g, oc, x, z, o)))))
        cn_own[g, x, zz] = norm(rounded)
    for j, (d, dg, dx, cp) in enumerate(gather_b):
        cp.wait_recv()
        zz, gg, xx = down(z, d, Z), down(g, dg, G), down(x, dx, X)
        i = 1 + j % len(plane)
        if C > 1:
            if dg:
                src, dst = r_own.at[gg, xx, zz], r_oth.at[gg, xx, zz]
            else:
                src, dst = f_own.at[xx, zz], f_oth.at[xx, zz]
            gather_a.append((d, dg, dx, go(remote(src, dst, sga.at[d, i], rga.at[d, i], at(g, oc, x, z, o)))))
        if dg == 0:
            r_own[g, xx, zz] = f_own[xx, zz].astype(jnp.bfloat16)
        cn_own[gg, xx, zz] = norm(r_own[gg, xx, zz])

    def nearest(r_buf, cn_buf, first):
        for b in range(nblk):
            gb = route_ref[b]
            cen = r_buf[gb].reshape(half, D)
            cn = cn_buf[gb].reshape(half, D)
            cross = lax.dot_general(cen, pts_ref[b * width:(b + 1) * width, :], (((1,), (1,)), ((), ())),
                                    preferred_element_type=jnp.float32)
            low = jnp.min(cn - (2.0 / D) * cross, axis=0, keepdims=True)
            if first:
                dist_ref[b:b + 1, :] = low
            else:
                dist_ref[b:b + 1, :] = jnp.minimum(dist_ref[b:b + 1, :], low)

    nearest(r_own, cn_own, True)
    cent_ref[c] = f_own[...]
    if C > 1:
        for d, dg, dx, cp in gather_a:
            cp.wait_recv()
            zz, gg, xx = down(z, d, Z), down(g, dg, G), down(x, dx, X)
            if dg == 0:
                r_oth[g, xx, zz] = f_oth[xx, zz].astype(jnp.bfloat16)
            cn_oth[gg, xx, zz] = norm(r_oth[gg, xx, zz])
        nearest(r_oth, cn_oth, False)
    dist = dist_ref[...] + xn[...]
    dist_ref[...] = dist
    ibuf[me] = jnp.sum(dist, axis=0, keepdims=True)

    def tell(i):
        t = lax.rem(me + i, n)
        return remote(ibuf.at[me], ibuf.at[me], si.at[i], ri.at[i], (t // S, lax.rem(t, S)))

    def start(i, _):
        tell(i).start()
        return 0

    def finish(i, _):
        tell(i).wait()
        return 0

    lax.fori_loop(1, n, start, 0)
    if C > 1:
        cent_ref[oc] = f_oth[...]
    for cp in sent:
        cp.wait_send()
    lax.fori_loop(1, n, finish, 0)
    inert_ref[...] = jnp.sum(jnp.sum(ibuf[...], axis=0), axis=1, keepdims=True) / total_points


def per_device(G, S, points, sub_label, block_route):
    C, X, Z, O = plan(S)
    N, D = points.shape
    nblk = block_route.shape[0]
    width = N // nblk
    R = K // (C * X * Z)
    f32, bf16 = jnp.float32, jnp.bfloat16
    V = pltpu.VMEM
    dma = pltpu.SemaphoreType.DMA
    rp = R + 8
    peers = max(G * X - 1, 1)
    zs, os_ = max(Z - 1, 1), max(O - 1, 1)
    vmem = pl.BlockSpec(memory_space=pltpu.VMEM)
    cent, dist, inert = pl.pallas_call(
        functools.partial(kernel, (G, S, C, X, Z, O, R)),
        out_shape=(
            jax.ShapeDtypeStruct((C, X, Z, R, D), f32),
            jax.ShapeDtypeStruct((nblk, width), f32),
            jax.ShapeDtypeStruct((1, 1), f32),
        ),
        in_specs=[pl.BlockSpec(memory_space=pltpu.SMEM), vmem, vmem],
        out_specs=(vmem, vmem, vmem),
        scratch_shapes=[
            V((N, 2 * D), bf16), V((G * X * Z * R, N), bf16),
            V((C, G, X, Z, rp, D), f32), V((G, X, Z, rp, D), f32),
            V((peers, Z, rp, D), f32), V((zs, rp, D), f32),
            V((rp, D), f32), V((os_, rp, D), f32),
            V((X, Z, R, D), f32), V((X, Z, R, D), f32),
            V((G, X, Z, R, D), bf16), V((G, X, Z, R, D), bf16),
            V((G, X, Z, R, D), f32), V((G, X, Z, R, D), f32),
            V((nblk, width), f32), V((G * S, 1, width), f32),
            dma, dma, dma((peers,)), dma((peers,)), dma((zs,)), dma((zs,)),
            dma((os_,)), dma((os_,)), dma((zs,)), dma((zs,)),
            dma((Z, peers)), dma((Z, peers)), dma((Z, peers + 1)), dma((Z, peers + 1)),
            dma((G * S,)), dma((G * S,)),
        ],
        compiler_params=pltpu.CompilerParams(collective_id=0, has_side_effects=True, vmem_limit_bytes=48 * 2**20),
    )(block_route[:, 0], points, sub_label.reshape(nblk, width))
    return cent.reshape(1, K, D), dist.reshape(N), inert.reshape(())


def solution(mesh):
    placed = (P(("grp", "shard"), None), P(("grp", "shard")), P(("grp", "shard"), None))
    return jax.shard_map(
        functools.partial(per_device, mesh.shape["grp"], mesh.shape["shard"]),
        mesh=mesh,
        in_specs=placed,
        out_specs=(P("grp", None, None), P(("grp", "shard")), P()),
        check_vma=False,
    )
```
